32 devices in a mesh: fsdp: 4 (over y, x), ctx: 8 (over z, core).
Axes of the slice: x: 2, y: 2, z: 4, core: 2. Of those that a mesh axis runs over, the one named last changes fastest.
Arguments:
- layer_input: bfloat16 [4, 1024, 1600], P('fsdp', 'ctx'), may hold values from -6 to 6
- pair_blocks: int32 [8, 2], replicated, may hold values from 0 to 15, as said below
- ln1_gain: bfloat16 [1600], P('fsdp'), may hold values from 0.25 to 1.75
- ln1_bias: bfloat16 [1600], P('fsdp'), may hold values from -3 to 3
- w_qkv: bfloat16 [1600, 4800], P('fsdp'), may hold values from -0.15625 to 0.15625
- bias_q: bfloat16 [1600], P('fsdp'), may hold values from -5 to 5
- bias_v: bfloat16 [1600], P('fsdp'), may hold values from -3 to 3
- w_proj: bfloat16 [1600, 1600], P('fsdp'), may hold values from -0.625 to 0.625
- bias_proj: bfloat16 [1600], P('fsdp'), may hold values from -3 to 3
- ln2_gain: bfloat16 [1600], P('fsdp'), may hold values from 0.25 to 1.75
- ln2_bias: bfloat16 [1600], P('fsdp'), may hold values from -3 to 3
- w_fc: bfloat16 [1600, 6400], P('fsdp'), may hold values from -0.15625 to 0.15625
- bias_fc: bfloat16 [6400], P('fsdp'), may hold values from -3 to 3
- w_out: bfloat16 [6400, 1600], P('fsdp'), may hold values from -0.078125 to 0.078125
- bias_out: bfloat16 [1600], P('fsdp'), may hold values from -3 to 3
- cotangent: bfloat16 [4, 1024, 1600], P('fsdp', 'ctx'), may hold values from -6 to 6
Outputs:
- output: bfloat16 [4, 1024, 1600], P('fsdp', 'ctx')
- grad_input: bfloat16 [4, 1024, 1600], P('fsdp', 'ctx')
- grad_ln1_gain: float32 [1600], P('fsdp')
- grad_ln1_bias: float32 [1600], P('fsdp')
- grad_w_qkv: float32 [1600, 4800], P('fsdp')
- grad_bias_q: float32 [1600], P('fsdp')
- grad_bias_v: float32 [1600], P('fsdp')
- grad_w_proj: float32 [1600, 1600], P('fsdp')
- grad_bias_proj: float32 [1600], P('fsdp')
- grad_ln2_gain: float32 [1600], P('fsdp')
- grad_ln2_bias: float32 [1600], P('fsdp')
- grad_w_fc: float32 [1600, 6400], P('fsdp')
- grad_bias_fc: float32 [6400], P('fsdp')
- grad_w_out: float32 [6400, 1600], P('fsdp')
- grad_bias_out: float32 [1600], P('fsdp')
The draws below stay inside these ranges and needn't reach their ends.
Inputs may be any that keep to these rules, and one draw needn't show every extreme that they name: `pair_blocks`: row r is b and 15 - b for some b < 8; the first entries of the rows are a permutation of 0 to 7.
All inputs are finite; a program needn't handle non-finite values.
Results may differ from the reference program's by a relative error of at most 0.017.
Values may be sent and summed in bfloat16 or wider, within the bound.
A program may use at most 384 MiB of HBM per device.

```python
from functools import partial
import jax
import jax.numpy as jnp
from jax import lax

D = 1600
HEADS = 25
HEAD = 64
FF = 6400
BLK = 64
LEN = 1024
SEQS = 4
N_CTX = 8


def draw_pair_blocks(key, part):
    first = jax.random.permutation(key, N_CTX).astype(jnp.int32)
    return jnp.stack([first, 2 * N_CTX - 1 - first], axis=1).astype(jnp.int32)


def shard_levels(own_key, shape, cuts, least, largest):
    def one(position, parts):
        steps = jax.random.uniform(jax.random.fold_in(jax.random.fold_in(own_key, 6), position), (parts,), jnp.float32, least / len(cuts), largest / len(cuts))
        return jnp.repeat(jnp.exp(steps), shape[position] // parts).reshape((-1,) + (1,) * (len(shape) - position - 1))

    loudness = one(*cuts[0])
    for cut in cuts[1:]:
        loudness = loudness * one(*cut)
    return loudness


def bell_draw(own_key, extent, deviation, reach, cuts=(), kind=jnp.bfloat16):
    values = jax.random.normal(own_key, extent, jnp.float32) * deviation
    if len(cuts) > 0:
        values = shard_levels(own_key, extent, cuts, -0.22, 0.18) * values
    return jnp.clip(values, min=-reach, max=reach).astype(kind)


def setup_inputs(seed: int = 0) -> dict:
    streams_of = jax.random.split(jax.random.key(seed), 17)
    layer_input = bell_draw(streams_of[0], (SEQS, LEN, D), 1.0, 6.0, ((0, 4), (1, 8)))
    pair_blocks = draw_pair_blocks(jax.random.fold_in(streams_of[16], 71), 0)
    ln1_gain = jnp.clip(1.0 + 0.15 * jax.random.normal(streams_of[2], (D,), jnp.float32), 0.25, 1.75).astype(jnp.bfloat16)
    ln1_bias = bell_draw(streams_of[3], (D,), 0.5, 3.0, ((0, 4),))
    w_qkv = bell_draw(streams_of[4], (D, 3 * D), D ** -0.5, 0.15625, ((0, 4),))
    bias_q = bell_draw(streams_of[5], (D,), 1.0, 5.0, ((0, 4),))
    bias_v = bell_draw(streams_of[6], (D,), 0.5, 3.0, ((0, 4),))
    w_proj = bell_draw(streams_of[7], (D, D), (D // 16) ** -0.5, 0.625, ((0, 4),))
    bias_proj = bell_draw(streams_of[8], (D,), 0.5, 3.0, ((0, 4),))
    ln2_gain = jnp.clip(1.0 + 0.15 * jax.random.normal(streams_of[9], (D,), jnp.float32), 0.25, 1.75).astype(jnp.bfloat16)
    ln2_bias = bell_draw(streams_of[10], (D,), 0.5, 3.0, ((0, 4),))
    w_fc = bell_draw(streams_of[11], (D, FF), D ** -0.5, 0.15625, ((0, 4),))
    bias_fc = bell_draw(streams_of[12], (FF,), 0.5, 3.0, ((0, 4),))
    w_out = bell_draw(streams_of[13], (FF, D), FF ** -0.5, 0.078125, ((0, 4),))
    bias_out = bell_draw(streams_of[14], (D,), 0.5, 3.0, ((0, 4),))
    cotangent = bell_draw(streams_of[15], (SEQS, LEN, D), 1.0, 6.0, ((0, 4), (1, 8)))
    return dict(layer_input=layer_input, pair_blocks=pair_blocks, ln1_gain=ln1_gain, ln1_bias=ln1_bias, w_qkv=w_qkv, bias_q=bias_q, bias_v=bias_v, w_proj=w_proj, bias_proj=bias_proj, ln2_gain=ln2_gain, ln2_bias=ln2_bias, w_fc=w_fc, bias_fc=bias_fc, w_out=w_out, bias_out=bias_out, cotangent=cotangent)


EPSILON = 1e-05
HIGHEST = lax.Precision.HIGHEST

@jax.custom_vjp
def low(v):
    return lax.optimization_barrier(v.astype(jnp.bfloat16)).astype(jnp.float32)

@jax.custom_vjp
def low_back(v):
    return v

def low_keep(v):
    return (low(v), None)

def low_pass(kept, grad):
    return (grad,)

def back_keep(v):
    return (v, None)

def back_low(kept, grad):
    return (low(grad),)
low.defvjp(low_keep, low_pass)
low_back.defvjp(back_keep, back_low)

def matmul(left, right):
    return jnp.dot(left, right, precision=HIGHEST, preferred_element_type=jnp.float32)

def layer_norm(inputs, gain, shift):
    centred = inputs - lax.optimization_barrier(jnp.mean(inputs, axis=-1, keepdims=True))
    inverse = lax.rsqrt(lax.optimization_barrier(jnp.mean(centred * centred, axis=-1, keepdims=True)) + EPSILON)
    return centred * inverse * gain + shift

def attention(query, key_rows, value_rows, positions):
    length = query.shape[0]
    block_rows = min(512, length)
    query_blocks = query.reshape(length // block_rows, block_rows, HEADS, HEAD)
    position_blocks = positions.reshape(length // block_rows, block_rows)
    key_heads = key_rows.reshape(length, HEADS, HEAD)
    value_heads = value_rows.reshape(length, HEADS, HEAD)

    def one_block(pieces):
        query_block, position_block = pieces
        score = low_back(jnp.einsum('qhe,khe->hqk', query_block, key_heads, precision=HIGHEST))
        allowed = position_block[None, :, None] >= positions[None, None, :]
        score = jnp.where(allowed, score, -jnp.inf)
        weights = low(jax.nn.softmax(score, axis=-1))
        return jnp.einsum('hqk,khe->qhe', weights, value_heads, precision=HIGHEST)
    result = lax.map(jax.checkpoint(one_block), (query_blocks, position_blocks))
    return result.reshape(length, HEADS * HEAD)

def forward(positions, stream, ln1_gain, ln1_bias, w_qkv, bias_q, bias_v, w_proj, bias_proj, ln2_gain, ln2_bias, w_fc, bias_fc, w_out, bias_out):
    flat = stream.reshape(SEQS * LEN, D)
    normed_one = low(layer_norm(flat, ln1_gain, ln1_bias))
    projected = matmul(normed_one, w_qkv)
    query = low_back(low((projected[:, :D] + bias_q) * HEAD ** (-0.5)))
    key_rows = low_back(low(projected[:, D:2 * D]))
    value_rows = low_back(low(projected[:, 2 * D:] + bias_v))

    def per_sequence(pieces):
        return attention(pieces[0], pieces[1], pieces[2], positions)
    context = lax.map(per_sequence, (query.reshape(SEQS, LEN, D), key_rows.reshape(SEQS, LEN, D), value_rows.reshape(SEQS, LEN, D)))
    context = low_back(low(context.reshape(SEQS * LEN, D)))
    attended = low_back(matmul(context, w_proj) + bias_proj)
    mixed = flat + attended
    normed_two = low(layer_norm(mixed, ln2_gain, ln2_bias))
    hidden = low_back(matmul(normed_two, w_fc) + bias_fc)
    activated = low(jax.nn.gelu(hidden, approximate=True))
    branch = low_back(matmul(activated, w_out) + bias_out)
    return (mixed + branch).reshape(SEQS, LEN, D)

def reference(layer_input, pair_blocks, ln1_gain, ln1_bias, w_qkv, bias_q, bias_v, w_proj, bias_proj, ln2_gain, ln2_bias, w_fc, bias_fc, w_out, bias_out, cotangent):
    offsets = jnp.arange(BLK, dtype=jnp.int32)
    positions = (pair_blocks.astype(jnp.int32)[:, :, None] * BLK + offsets[None, None, :]).reshape(LEN).astype(jnp.int32)
    result, pullback = jax.vjp(partial(forward, positions), layer_input.astype(jnp.float32), ln1_gain.astype(jnp.float32), ln1_bias.astype(jnp.float32), w_qkv.astype(jnp.float32), bias_q.astype(jnp.float32), bias_v.astype(jnp.float32), w_proj.astype(jnp.float32), bias_proj.astype(jnp.float32), ln2_gain.astype(jnp.float32), ln2_bias.astype(jnp.float32), w_fc.astype(jnp.float32), bias_fc.astype(jnp.float32), w_out.astype(jnp.float32), bias_out.astype(jnp.float32))
    grads = pullback(cotangent.astype(jnp.float32))
    return (result.astype(jnp.bfloat16), grads[0].astype(jnp.bfloat16), grads[1], grads[2], grads[3], grads[4], grads[5], grads[6], grads[7], grads[8], grads[9], grads[10], grads[11], grads[12], grads[13])
```

```python
from functools import partial

import jax
import jax.numpy as jnp
from jax import lax
from jax.experimental import pallas as pl
from jax.experimental.pallas import tpu as pltpu
from jax.sharding import PartitionSpec as P

HEADS = 25
HEAD = 64
EPSILON = 1e-05
MASKED = -1e30
BF = jnp.bfloat16
F32 = jnp.float32
BQ = 256


def matmul(left, right):
    return jnp.dot(left, right, preferred_element_type=F32)


def matmul_t(left, right):
    return lax.dot_general(left, right, (((1,), (1,)), ((), ())), preferred_element_type=F32)


def t_matmul(left, right):
    return lax.dot_general(left, right, (((0,), (0,)), ((), ())), preferred_element_type=F32)


def normalize(inputs):
    centred = inputs - jnp.mean(inputs, axis=-1, keepdims=True)
    inverse = lax.rsqrt(jnp.mean(centred * centred, axis=-1, keepdims=True) + EPSILON)
    return centred * inverse, inverse


def norm_back(grad_out, normed, inverse, gain):
    grad_norm = grad_out * gain
    mean_grad = jnp.mean(grad_norm, axis=-1, keepdims=True)
    mean_dot = jnp.mean(grad_norm * normed, axis=-1, keepdims=True)
    return inverse * (grad_norm - mean_grad - normed * mean_dot)


def gelu_pair(v):
    a = 0.7978845608028654
    inner = a * (v + 0.044715 * v * v * v)
    t = jnp.tanh(inner)
    value = 0.5 * v * (1.0 + t)
    slope = 0.5 * (1.0 + t) + 0.5 * v * (1.0 - t * t) * a * (1.0 + 3 * 0.044715 * v * v)
    return value, slope


def head_mask(width, head):
    lane = lax.broadcasted_iota(jnp.int32, (1, width), 1)
    return (lane >= head * HEAD) & (lane < (head + 1) * HEAD)


def sort_in(where_ref, blocks, blk, src, dst):
    for b in range(blocks):
        at = pl.multiple_of(where_ref[b] * blk, blk)
        dst[b * blk : (b + 1) * blk, :] = src[pl.ds(at, blk), :]


def each_block(length, step):
    if length <= 1024:
        for i in range(length // BQ):
            step(i * BQ, (i + 1) * BQ)
    else:
        pl.loop(0, length // BQ)(lambda i: step(pl.multiple_of(i * BQ, BQ), length))


def attend_kernel(blocks, blk, where_ref, q_ref, k_ref, v_ref, o_ref, lse_ref, q_s, k_s, v_s, o_s):
    length, width = q_ref.shape
    sort_in(where_ref, blocks, blk, q_ref, q_s)
    sort_in(where_ref, blocks, blk, k_ref, k_s)
    sort_in(where_ref, blocks, blk, v_ref, v_s)
    def step(base, ext):
        row = lax.broadcasted_iota(jnp.int32, (BQ, ext), 0) + base
        col = lax.broadcasted_iota(jnp.int32, (BQ, ext), 1)
        seen = col <= row
        now = pl.ds(base, BQ)
        q = q_s[now, :]
        total = None
        for h in range(width // HEAD):
            mine = head_mask(width, h)
            score = matmul_t(jnp.where(mine, q, 0).astype(BF), k_s[:ext, :])
            score = jnp.where(seen, score, MASKED)
            top = jnp.max(score, axis=1, keepdims=True)
            prob = jnp.exp(score - top)
            norm = jnp.sum(prob, axis=1, keepdims=True)
            out = matmul(prob.astype(BF), v_s[:ext, :]) / norm
            total = out if total is None else jnp.where(mine, out, total)
            lse = jnp.broadcast_to(top + jnp.log(norm), (BQ, 128))
            lse_ref[0, h : h + 1, now] = jnp.transpose(lse)[0:1, :]
        o_s[now, :] = total.astype(BF)

    each_block(length, step)
    for b in range(blocks):
        at = pl.multiple_of(where_ref[b] * blk, blk)
        o_ref[pl.ds(at, blk), :] = o_s[b * blk : (b + 1) * blk, :]


def attend_back_kernel(
    blocks, blk, where_ref, q_ref, k_ref, v_ref, g_ref, lse_ref, dq_ref, dk_ref, dv_ref,
    q_s, k_s, v_s, g_s, dq_s, dk_s, dv_s,
):
    length, width = q_ref.shape
    sort_in(where_ref, blocks, blk, q_ref, q_s)
    sort_in(where_ref, blocks, blk, k_ref, k_s)
    sort_in(where_ref, blocks, blk, v_ref, v_s)
    sort_in(where_ref, blocks, blk, g_ref, g_s)
    dk_s[...] = jnp.zeros_like(dk_s)
    dv_s[...] = jnp.zeros_like(dv_s)

    def step(base, ext):
        key = lax.broadcasted_iota(jnp.int32, (ext, BQ), 0)
        query = lax.broadcasted_iota(jnp.int32, (ext, BQ), 1) + base
        seen = key <= query
        now = pl.ds(base, BQ)
        q = q_s[now, :]
        g = g_s[now, :]
        dq_total = None
        for h in range(width // HEAD):
            mine = head_mask(width, h)
            q_h = jnp.where(mine, q, 0).astype(BF)
            g_h = jnp.where(mine, g, 0).astype(BF)
            score = matmul_t(k_s[:ext, :], q_h)
            prob = jnp.where(seen, jnp.exp(score - lse_ref[0, h : h + 1, now]), 0.0)
            grad_prob = matmul_t(v_s[:ext, :], g_h)
            delta = jnp.sum(prob * grad_prob, axis=0, keepdims=True)
            grad_score = (prob * (grad_prob - delta)).astype(BF)
            dv_s[:ext, :] += matmul(prob.astype(BF), g_h)
            dk_s[:ext, :] += matmul(grad_score, q_h)
            dq = t_matmul(grad_score, k_s[:ext, :])
            dq_total = dq if dq_total is None else jnp.where(mine, dq, dq_total)
        dq_s[now, :] = dq_total

    each_block(length, step)
    for b in range(blocks):
        at = pl.multiple_of(where_ref[b] * blk, blk)
        dq_ref[pl.ds(at, blk), :] = dq_s[b * blk : (b + 1) * blk, :].astype(BF)
        dk_ref[pl.ds(at, blk), :] = dk_s[b * blk : (b + 1) * blk, :].astype(BF)
        dv_ref[pl.ds(at, blk), :] = dv_s[b * blk : (b + 1) * blk, :].astype(BF)


def attention_specs(length, slots, blocks):
    width = 128 if slots % 2 == 0 else slots * HEAD
    groups = slots * HEAD // width
    part = lambda offset: pl.BlockSpec((length, width), lambda g, where: (0, offset * groups + g))
    lse = pl.BlockSpec((1, 8, length), lambda g, where: (g, 0, 0))
    return width, groups, part, lse


def attend(where, qkv, slots, blk):
    length = qkv.shape[0]
    blocks = length // blk
    width, groups, part, lse = attention_specs(length, slots, blocks)
    return pl.pallas_call(
        partial(attend_kernel, blocks, blk),
        out_shape=(
            jax.ShapeDtypeStruct((length, slots * HEAD), BF),
            jax.ShapeDtypeStruct((groups, 8, length), F32),
        ),
        grid_spec=pltpu.PrefetchScalarGridSpec(
            num_scalar_prefetch=1,
            grid=(groups,),
            in_specs=[part(0), part(1), part(2)],
            out_specs=[part(0), lse],
            scratch_shapes=[pltpu.VMEM((length, width), BF)] * 4,
        ),
        compiler_params=pltpu.CompilerParams(vmem_limit_bytes=60 << 20),
        cost_estimate=pl.CostEstimate(
            flops=4 * slots * length * length * HEAD,
            transcendentals=slots * length * length,
            bytes_accessed=8 * length * slots * HEAD,
        ),
        name="attend",
    )(where, qkv, qkv, qkv)


def attend_back(where, qkv, grad, lse_rows, slots, blk):
    length = qkv.shape[0]
    blocks = length // blk
    width, groups, part, lse = attention_specs(length, slots, blocks)
    return pl.pallas_call(
        partial(attend_back_kernel, blocks, blk),
        out_shape=(jax.ShapeDtypeStruct((length, slots * HEAD), BF),) * 3,
        grid_spec=pltpu.PrefetchScalarGridSpec(
            num_scalar_prefetch=1,
            grid=(groups,),
            in_specs=[part(0), part(1), part(2), part(0), lse],
            out_specs=[part(0)] * 3,
            scratch_shapes=[pltpu.VMEM((length, width), BF)] * 4
            + [pltpu.VMEM((length, width), F32)] * 3,
        ),
        compiler_params=pltpu.CompilerParams(vmem_limit_bytes=60 << 20),
        cost_estimate=pl.CostEstimate(
            flops=10 * slots * length * length * HEAD,
            transcendentals=slots * length * length,
            bytes_accessed=14 * length * slots * HEAD,
        ),
        name="attend_back",
    )(where, qkv, qkv, qkv, grad, lse_rows)


def shards(
    m,
    n,
    layer_input,
    pair_blocks,
    ln1_gain,
    ln1_bias,
    w_qkv,
    bias_q,
    bias_v,
    w_proj,
    bias_proj,
    ln2_gain,
    ln2_bias,
    w_fc,
    bias_fc,
    w_out,
    bias_out,
    cotangent,
):
    rows = layer_input.shape[1]
    width = layer_input.shape[2]
    length = rows * n
    blk = rows // 2
    units = w_out.shape[0]
    own_rows = w_qkv.shape[0]
    scale = HEAD ** (-0.5)
    f = lax.axis_index("fsdp")
    c = lax.axis_index("ctx")

    def swap_f(v, mask):
        return lax.ppermute(v, "fsdp", [(i, i ^ mask) for i in range(m)]) if mask else v

    def gather_f(v):
        return [swap_f(v, mask) for mask in range(m)]

    def settle_f(pieces):
        size = pieces[0].shape[0]
        whole = jnp.zeros((m * size,) + pieces[0].shape[1:], pieces[0].dtype)
        for mask, piece in enumerate(pieces):
            whole = lax.dynamic_update_slice_in_dim(whole, piece, (f ^ mask) * size, 0)
        return whole

    def sum_f(total):
        result = total[:rows]
        for mask in range(1, m):
            sent = total[mask * rows : (mask + 1) * rows].astype(BF)
            result = result + swap_f(sent, mask).astype(F32)
        return result

    slots = 2 * -(-HEADS // (2 * n))
    span = slots * HEAD
    bounds = [HEADS * i // n for i in range(n + 1)]
    starts = [min(bounds[i], HEADS - slots) for i in range(n)]
    kept = [
        slice((bounds[i] - starts[i]) * HEAD, (bounds[i + 1] - starts[i]) * HEAD) for i in range(n)
    ]
    holders = [i for i in range(n) if bounds[i + 1] > bounds[i]]
    first = jnp.minimum(HEADS * c // n, HEADS - slots)
    head = first + lax.broadcasted_iota(jnp.int32, (1, span), 1) // HEAD
    owned = ((head >= HEADS * c // n) & (head < HEADS * (c + 1) // n)).astype(F32)

    blocks = 2 * n
    flat = pair_blocks.reshape(-1)
    index = jnp.arange(blocks, dtype=jnp.int32)
    where = jnp.sum(jnp.where(flat[None, :] == index[:, None], index[None, :], 0), axis=1)

    x = layer_input[0]
    cot = cotangent[0]
    small = jnp.stack(
        [ln1_gain, ln1_bias, bias_q, bias_v, bias_proj, ln2_gain, ln2_bias, bias_out]
    )
    small = settle_f([v[None] for v in gather_f(small)])
    small = jnp.transpose(small, (1, 0, 2)).reshape(8, width).astype(F32)
    gain_one, shift_one, all_bias_q, all_bias_v, all_bias_proj, gain_two, shift_two, all_bias_out = (
        small[i] for i in range(8)
    )
    slice_qkv = lax.dynamic_slice_in_dim(
        w_qkv.reshape(own_rows, 3, width), first * HEAD, span, 2
    ).reshape(own_rows, 3 * span)
    head_qkv = lax.all_gather(slice_qkv, "fsdp", axis=0, tiled=True)
    head_bias_q = lax.dynamic_slice_in_dim(all_bias_q, first * HEAD, span, 0)
    head_bias_v = lax.dynamic_slice_in_dim(all_bias_v, first * HEAD, span, 0)
    full_proj = lax.all_gather(w_proj, "fsdp", axis=0, tiled=True)
    unit_fc = settle_f(
        [
            swap_f(lax.dynamic_slice_in_dim(w_fc, (f ^ mask) * units, units, 1), mask)
            for mask in range(m)
        ]
    )
    cots = jnp.concatenate(gather_f(cot), axis=0)

    all_x = lax.all_gather(x, "ctx", axis=0, tiled=True).astype(F32)
    h1 = (normalize(all_x)[0] * gain_one + shift_one).astype(BF)
    projected = matmul(h1, head_qkv)
    qkv = jnp.concatenate(
        [
            (projected[:, :span] + head_bias_q) * scale,
            projected[:, span : 2 * span],
            projected[:, 2 * span :] + head_bias_v,
        ],
        axis=1,
    ).astype(BF)
    head_context, lse = attend(where, qkv, slots, blk)
    sent = lax.all_to_all(head_context.reshape(n, rows, span), "ctx", 0, 0)
    context = jnp.concatenate(
        [sent[i][:, kept[i]] for i in holders], axis=1
    )
    xs = x.astype(F32)
    mixed = xs + (matmul(context, full_proj) + all_bias_proj)

    normed_two, inverse_two = normalize(mixed)
    h2 = (normed_two * gain_two + shift_two).astype(BF)
    h2s = jnp.concatenate(gather_f(h2), axis=0)
    hidden = matmul(h2s, unit_fc) + bias_fc.astype(F32)
    value, slope = gelu_pair(hidden)
    activated = value.astype(BF)
    result = (mixed + sum_f(matmul(activated, w_out)) + all_bias_out).astype(BF)

    grad_hidden = (matmul_t(cots, w_out) * slope).astype(BF)
    grad_h2 = sum_f(matmul_t(grad_hidden, unit_fc))
    grad_w_out = t_matmul(activated, cots).astype(BF)
    grad_w_fc = t_matmul(h2s, grad_hidden).astype(BF)
    grad_bias_fc = jnp.sum(grad_hidden.astype(F32), axis=0)
    grad_mixed = cot.astype(F32) + norm_back(grad_h2, normed_two, inverse_two, gain_two)

    part_out = lax.psum_scatter(grad_w_out, "ctx", scatter_dimension=0, tiled=True)
    out_grad_w_out = lax.all_gather(part_out, "ctx", axis=0, tiled=True).astype(F32)
    part_fc = lax.psum_scatter(grad_w_fc, "ctx", scatter_dimension=0, tiled=True)
    share = n // m
    route = [
        (i * n + j, (j // share) * n + i * share + j % share) for i in range(m) for j in range(n)
    ]
    part_fc = lax.ppermute(part_fc, ("fsdp", "ctx"), route)
    all_fc = lax.all_gather(part_fc, "ctx", axis=0, tiled=False)
    all_fc = all_fc.reshape(m, share, width // n, units).transpose(1, 2, 0, 3)
    out_grad_w_fc = all_fc.reshape(own_rows, m * units).astype(F32)

    grad_attended = grad_mixed.astype(BF)
    grad_context = matmul_t(grad_attended, full_proj).astype(BF)
    sent_back = jnp.stack(
        [grad_context[:, starts[i] * HEAD : starts[i] * HEAD + span] for i in range(n)]
    )
    grad_heads = lax.all_to_all(sent_back, "ctx", 0, 0).reshape(length, span)
    grad_heads = (grad_heads * owned.astype(BF)).astype(BF)
    grad_query, grad_keys, grad_values = attend_back(where, qkv, grad_heads, lse, slots, blk)
    grad_qkv = jnp.concatenate([grad_query * BF(scale), grad_keys, grad_values], axis=1)

    rows_proj = jnp.concatenate(
        [
            swap_f(lax.dynamic_slice_in_dim(context, (f ^ mask) * own_rows, own_rows, 1), mask)
            for mask in range(m)
        ],
        axis=0,
    )
    grad_w_proj = t_matmul(rows_proj, jnp.concatenate(gather_f(grad_attended), axis=0)).astype(BF)
    out_grad_w_proj = lax.psum(grad_w_proj, "ctx").astype(F32)

    partial_h1 = matmul_t(grad_qkv, head_qkv)
    grad_h1 = lax.psum_scatter(partial_h1.astype(BF), "ctx", scatter_dimension=0, tiled=True)
    grad_h1 = grad_h1.astype(F32)
    normed_one, inverse_one = normalize(xs)
    grad_stream = grad_mixed + norm_back(grad_h1, normed_one, inverse_one, gain_one)

    grad_head_qkv = t_matmul(h1, grad_qkv)
    mine = lax.psum_scatter(grad_head_qkv.astype(BF), "fsdp", scatter_dimension=0, tiled=True)
    gathered = lax.all_gather(mine, "ctx", axis=0, tiled=False).reshape(n, own_rows, 3, span)
    out_grad_w_qkv = jnp.concatenate(
        [
            gathered[i, :, kind, kept[i]]
            for kind in range(3)
            for i in holders
        ],
        axis=1,
    ).astype(F32)

    def spread(v):
        whole = jnp.zeros((width,), F32)
        return lax.dynamic_update_slice_in_dim(whole, v * owned[0], first * HEAD, 0)

    sums = jnp.stack(
        [
            jnp.sum(grad_h1 * normed_one, axis=0),
            jnp.sum(grad_h1, axis=0),
            spread(jnp.sum(grad_query.astype(F32), axis=0) * scale),
            spread(jnp.sum(grad_values.astype(F32), axis=0)),
            jnp.sum(grad_attended.astype(F32), axis=0),
            jnp.sum(grad_h2 * normed_two, axis=0),
            jnp.sum(grad_h2, axis=0),
            jnp.sum(cot.astype(F32), axis=0),
        ]
    )
    sums = lax.psum(sums, ("fsdp", "ctx"))
    sums = lax.dynamic_slice_in_dim(sums, f * own_rows, own_rows, 1)
    out_bias_fc = lax.psum(grad_bias_fc, "ctx")
    return (
        result[None],
        grad_stream.astype(BF)[None],
        sums[0],
        sums[1],
        out_grad_w_qkv,
        sums[2],
        sums[3],
        out_grad_w_proj,
        sums[4],
        sums[5],
        sums[6],
        out_grad_w_fc,
        out_bias_fc,
        out_grad_w_out,
        sums[7],
    )


def solution(mesh):
    tokens = P("fsdp", "ctx", None)
    vector = P("fsdp")
    matrix = P("fsdp", None)
    in_specs = (
        (tokens, P(), vector, vector, matrix, vector, vector, matrix, vector)
        + (vector, vector, matrix, vector, matrix, vector, tokens)
    )
    out_specs = (
        (tokens, tokens, vector, vector, matrix, vector, vector, matrix, vector)
        + (vector, vector, matrix, vector, matrix, vector)
    )
    body = partial(shards, mesh.shape["fsdp"], mesh.shape["ctx"])
    return jax.shard_map(
        body, mesh=mesh, in_specs=in_specs, out_specs=out_specs, check_vma=False
    )
```
